128 devices in a mesh: row: 16 (over z_lo, y, core), col: 8 (over x, z_hi).
Axes of the slice: x: 4, y: 4, z: 4 (z_hi: 2, z_lo: 2; z = z_hi * 2 + z_lo), core: 2. Of those that a mesh axis runs over, the one named last changes fastest.
Arguments:
- tokens: bfloat16 [2048, 12288], P('row', 'col'), may hold values from -10 to 10
- qkv_weight: bfloat16 [12288, 3, 8192], P('col', None, 'row'), as said below
- out_weight: bfloat16 [8192, 12288], P('row', 'col'), may hold values from -0.0625 to 0.0625
Outputs:
- mixed: bfloat16 [2048, 12288], P('row', 'col')
The draws below stay inside these ranges and needn't reach their ends.
Inputs may be any that keep to these rules, and one draw needn't show every extreme that they name: `qkv_weight`: entries of magnitude at most 3 / sqrt(12288).
All inputs are finite; a program needn't handle non-finite values.
Results may differ from the reference program's by a relative error of at most 0.0055.
Values may be sent and summed in bfloat16 or wider, within the bound.
No kernel may reach another device: no remote copies, remote signals or barrier semaphores. Data moves between devices by JAX's collectives and lax.ppermute only.
A program may use at most 128 MiB of HBM per device.

```python
import math
import jax
import jax.numpy as jnp
from jax import lax

D = 12288
HD = 128
HEADS = 64
SEQ = 2048
HW = 8192


def draw_tokens(key, part):
    base_key = jax.random.fold_in(key, 0)
    values = jnp.clip(jax.random.normal(base_key, (SEQ, D), jnp.float32), -6.0, 6.0)
    return values.astype(jnp.bfloat16)


def draw_qkv_weight(key, part):
    query_key, key_key, value_key = jax.random.split(key, 3)
    factor = 1.0 / jnp.sqrt(jnp.float32(D))
    shape = (D, HEADS * HD)
    query_part = jnp.clip(jax.random.normal(query_key, shape, jnp.float32), -3.0, 3.0)
    key_part = jnp.clip(jax.random.normal(key_key, shape, jnp.float32), -3.0, 3.0)
    value_part = jnp.clip(jax.random.normal(value_key, shape, jnp.float32), -3.0, 3.0)
    stacked = jnp.stack([query_part, key_part, value_part], axis=1) * factor
    return stacked.astype(jnp.bfloat16)


def steps_of(key, extent, pieces, least, top_value):
    factor_of, own = 1.0, jax.random.fold_in(key, 6)
    for position, blocks in pieces:
        draws = jnp.exp(jax.random.uniform(jax.random.fold_in(own, position), (blocks,), jnp.float32, least / len(pieces), top_value / len(pieces)))
        factor_of = factor_of * jnp.repeat(draws, extent[position] // blocks).reshape([-1 if axis == position else 1 for axis in range(len(extent))])
    return factor_of


def gaussian(rng, shape, spread, bound, cuts=(), kind=jnp.bfloat16):
    drawn = spread * jax.random.normal(rng, shape, jnp.float32)
    if cuts:
        drawn = drawn * steps_of(rng, shape, cuts, -0.22, 0.18)
    return jnp.clip(drawn, -bound, bound).astype(kind)


def setup_inputs(seed: int = 0) -> dict:
    seeds = jax.random.split(jax.random.key(seed), 4)
    return {
        "tokens": draw_tokens(jax.random.fold_in(seeds[3], 71), 0),
        "qkv_weight": draw_qkv_weight(jax.random.fold_in(seeds[3], 71), 0),
        "out_weight": gaussian(seeds[2], (HW, D), HW ** -0.5, 0.0625, ((0, 16), (1, 8))),
    }


def one_head(stacked):
    query_head, key_head, value_head = stacked
    scores = jnp.dot(query_head, key_head.T, preferred_element_type=jnp.float32) * (1.0 / math.sqrt(HD))
    positions = jnp.arange(SEQ, dtype=jnp.int32)
    causal = positions[:, None] >= positions[None, :]
    scores = jnp.where(causal, scores, -1e+30)
    top = lax.optimization_barrier(jnp.max(scores, axis=1, keepdims=True))
    weights = jnp.where(causal, jnp.exp(scores - top), 0.0)
    total = lax.optimization_barrier(jnp.sum(weights, axis=1, keepdims=True))
    context = jnp.dot(weights.astype(jnp.bfloat16), value_head, preferred_element_type=jnp.float32) / total
    return context

def reference(tokens, qkv_weight, out_weight):
    width = HEADS * HD
    weight_flat = qkv_weight.reshape(D, 3 * width)
    qkv = jnp.dot(tokens, weight_flat, preferred_element_type=jnp.float32).astype(jnp.bfloat16)
    qkv = qkv.reshape(SEQ, 3, HEADS, HD)
    queries = jnp.transpose(qkv[:, 0], (1, 0, 2))
    key_rows = jnp.transpose(qkv[:, 1], (1, 0, 2))
    value_rows = jnp.transpose(qkv[:, 2], (1, 0, 2))
    context = lax.map(one_head, (queries, key_rows, value_rows))
    context = jnp.transpose(context, (1, 0, 2)).reshape(SEQ, width).astype(jnp.bfloat16)
    branch = jnp.dot(context, out_weight, preferred_element_type=jnp.float32)
    return (tokens.astype(jnp.float32) + branch).astype(jnp.bfloat16)
```

```python
import math
from functools import partial

import jax
import jax.numpy as jnp
from jax import lax
from jax.experimental import pallas as pl
from jax.experimental.pallas import tpu as pltpu
from jax.sharding import Mesh, PartitionSpec as P

HD = 128
BLK = 128
HALF = 64
F32 = jnp.float32
BF16 = jnp.bfloat16
CHUNKS = (((0, 0),), ((1, 0), (0, 1), (0, 3)), ((0, 2), (1, 1), (1, 3)), ((1, 2),))
BLOCKS = tuple(b for chunk in CHUNKS for b in chunk)


def ring(n, step):
    return [(i, (i + step) % n) for i in range(n)]


def fetch(x, axis, n, step):
    return lax.ppermute(x, axis, ring(n, -step))


def push(x, axis, n, step):
    return lax.ppermute(x, axis, ring(n, step))


def swap(x, axis):
    return lax.ppermute(x, axis, ring(2, 1))


def copy_body(at_ref, in_ref, out_ref):
    out_ref[...] = in_ref[...].reshape(out_ref.shape)


def heads_first_own(weight, x):
    d = weight.shape[1]
    return pl.pallas_call(
        copy_body,
        grid_spec=pltpu.PrefetchScalarGridSpec(
            num_scalar_prefetch=1,
            grid=(4, 3),
            in_specs=[pl.BlockSpec((1, d, HD), lambda h, s, at: (s, 0, (at[0] + h) % 4))],
            out_specs=pl.BlockSpec((d, HD), lambda h, s, at: (0, 3 * h + s)),
        ),
        out_shape=jax.ShapeDtypeStruct((d, 12 * HD), weight.dtype),
        name="order_qkv",
    )(x, weight)


def rows_first_own(weight, x):
    n = weight.shape[1]
    return pl.pallas_call(
        copy_body,
        grid_spec=pltpu.PrefetchScalarGridSpec(
            num_scalar_prefetch=1,
            grid=(4,),
            in_specs=[pl.BlockSpec((HD, n), lambda h, at: ((at[0] + h) % 4, 0))],
            out_specs=pl.BlockSpec((HD, n), lambda h, at: (h, 0)),
        ),
        out_shape=jax.ShapeDtypeStruct(weight.shape, weight.dtype),
        name="order_out",
    )(x, weight)


def attend_body(q_ref, k_ref, v_ref, qpos_ref, kpos_ref, out_ref):
    scores = lax.dot_general(q_ref[...], k_ref[...], (((1,), (1,)), ((), ())), preferred_element_type=F32)
    causal = qpos_ref[...] >= kpos_ref[...]
    scores = jnp.where(causal, scores * (1.0 / math.sqrt(HD)), -1e30)
    top = jnp.max(scores, axis=1, keepdims=True)
    weights = jnp.exp(scores - top)
    total = jnp.sum(weights, axis=1, keepdims=True)
    update = jnp.dot(weights.astype(BF16), v_ref[...], preferred_element_type=F32)
    out_ref[...] = (update / total).astype(BF16)


def attention(q, k, v, qpos, kpos, tile=256):
    nq, nk = q.shape[0], k.shape[0]
    return pl.pallas_call(
        attend_body,
        grid=(nq // tile,),
        in_specs=[
            pl.BlockSpec((tile, HD), lambda i: (i, 0)),
            pl.BlockSpec((nk, HD), lambda i: (0, 0)),
            pl.BlockSpec((nk, HD), lambda i: (0, 0)),
            pl.BlockSpec((tile, 1), lambda i: (i, 0)),
            pl.BlockSpec((1, nk), lambda i: (0, 0)),
        ],
        out_specs=pl.BlockSpec((tile, HD), lambda i: (i, 0)),
        out_shape=jax.ShapeDtypeStruct((nq, HD), BF16),
        name="attend",
    )(q, k, v, qpos, kpos)


def gather_pairwise(own, ring_axis, n, pair_axis):
    got = {(0, 0): own}
    got[1, 0] = swap(own, pair_axis)
    got[0, 1] = fetch(own, ring_axis, n, 1)
    got[0, 3] = fetch(own, ring_axis, n, 3)
    got[0, 2] = fetch(own, ring_axis, n, 2)
    got[1, 1] = fetch(got[1, 0], ring_axis, n, 1)
    got[1, 3] = fetch(got[1, 0], ring_axis, n, 3)
    got[1, 2] = swap(got[0, 2], pair_axis)
    return got


def reduce_over_x(part):
    t = part.shape[0]
    w = part.shape[1] // 4
    b0, b1, b2, b3 = (part[:, i * w : (i + 1) * w] for i in range(4))
    up = push(b2[: t // 2].astype(BF16), "x", 4, 1).astype(F32)
    down = push(b2[t // 2 :].astype(BF16), "x", 4, -1).astype(F32)
    s1 = jnp.concatenate([b1[: t // 2] + up, b1[t // 2 :]]).astype(BF16)
    s3 = jnp.concatenate([b3[: t // 2], b3[t // 2 :] + down]).astype(BF16)
    r1 = push(s1, "x", 4, 1).astype(F32)
    r3 = push(s3, "x", 4, -1).astype(F32)
    return b0 + r1 + r3


def halves(q, zh):
    parts = q.reshape(-1, 2, HALF, q.shape[-1])
    low, high = parts[:, 0], parts[:, 1]
    own = jnp.where(zh == 0, low, high)
    other = jnp.where(zh == 0, high, low)
    return own.reshape(-1, q.shape[-1]), other.reshape(-1, q.shape[-1])


def reduce_over_zh(summed, zh):
    t = summed.shape[0]
    own_q, other_q = halves(summed[:, :HD], zh)
    k, v = summed[:, HD : 2 * HD], summed[:, 2 * HD :]
    sent = jnp.concatenate([k, v, other_q]).astype(BF16)
    got = swap(sent, "zh").astype(F32)
    k = (k + got[:t]).astype(BF16)
    v = (v + got[t : 2 * t]).astype(BF16)
    q = (own_q + got[2 * t :]).astype(BF16)
    return q, k, v


def reduce_over_rows(part):
    block = {b: part[i * HALF : (i + 1) * HALF] for i, b in enumerate(BLOCKS)}
    up = push(jnp.concatenate([block[0, 1], block[1, 1]]).astype(BF16), "y", 4, 1)
    down = push(jnp.concatenate([block[0, 3], block[1, 3]]).astype(BF16), "y", 4, -1)
    over = swap(block[1, 2].astype(BF16), "zl")
    far = push((block[0, 2] + over.astype(F32)).astype(BF16), "y", 4, 2)
    up, down = up.astype(F32), down.astype(F32)
    side = swap((block[1, 0] + up[HALF:] + down[HALF:]).astype(BF16), "zl")
    return block[0, 0] + up[:HALF] + down[:HALF] + far.astype(F32) + side.astype(F32)


def positions(zl, y, c, count, first):
    out = []
    for chunk in CHUNKS:
        for dc in range(2):
            for dz, dy in chunk:
                row = ((zl + dz) % 2) * 8 + ((y + dy) % 4) * 2 + (c + dc) % 2
                out.append(row * BLK + first + jnp.arange(count, dtype=jnp.int32))
    return jnp.concatenate(out)


def local(tokens, qkv_weight, out_weight):
    zl, y, c, x, zh = (lax.axis_index(a) for a in ("zl", "y", "c", "x", "zh"))
    at = x.reshape(1).astype(jnp.int32)
    w_qkv = heads_first_own(jnp.transpose(qkv_weight, (1, 0, 2)), at)
    w_own = rows_first_own(out_weight, at)
    w_other = swap(w_own, "c")
    w_out = jnp.concatenate([w.reshape(4, HD, -1) for w in (w_own, w_other)], axis=1)
    w_out = w_out.reshape(8 * HD, -1)

    rows = gather_pairwise(tokens, "y", 4, "zl")
    qs, ks, vs = [], [], []
    for chunk in CHUNKS:
        own = jnp.concatenate([rows[b] for b in chunk]) if len(chunk) > 1 else rows[chunk[0]]
        both = jnp.concatenate([own, swap(own, "c")])
        part = jnp.dot(both, w_qkv, preferred_element_type=F32)
        q, k, v = reduce_over_zh(reduce_over_x(part), zh)
        qs.append(q)
        ks.append(k)
        vs.append(v)
    qpos = positions(zl, y, c, HALF, zh * HALF)[:, None]
    kpos = positions(zl, y, c, BLK, 0)[None, :]
    context = attention(jnp.concatenate(qs), jnp.concatenate(ks), jnp.concatenate(vs), qpos, kpos)

    mine, theirs, first = [], [], 0
    for chunk in CHUNKS:
        n = len(chunk) * HALF
        mine.append(context[first : first + n])
        theirs.append(context[first + n : first + 2 * n])
        first += 2 * n
    pair = jnp.concatenate([jnp.concatenate(mine), swap(jnp.concatenate(theirs), "c")], axis=1)
    parts = gather_pairwise(pair, "x", 4, "zh")
    sums = []
    for side in range(2):
        lhs = jnp.concatenate([parts[side, i] for i in range(4)], axis=1)
        sums.append(reduce_over_rows(jnp.dot(lhs, w_out, preferred_element_type=F32)))
    low = jnp.where(zh == 0, sums[0], sums[1])
    high = jnp.where(zh == 0, sums[1], sums[0])
    return (tokens.astype(F32) + jnp.concatenate([low, high])).astype(BF16)


def solution(mesh):
    fine = Mesh(mesh.devices.reshape(2, 4, 2, 4, 2), ("zl", "y", "c", "x", "zh"))
    row, col = ("zl", "y", "c"), ("x", "zh")
    in_specs = (P(row, col), P(col, None, row), P(row, col))
    return jax.shard_map(local, mesh=fine, in_specs=in_specs, out_specs=P(row, col), check_vma=False)
```

```python
import math

import jax
import jax.numpy as jnp
from jax import lax
from jax.experimental import pallas as pl
from jax.experimental.pallas import tpu as pltpu
from jax.sharding import Mesh, PartitionSpec as P


HD = 128
BLK = 128
HALF = 64
F32 = jnp.float32
BF16 = jnp.bfloat16
CHUNKS = (((0, 0), (1, 0), (0, 1), (0, 3)), ((0, 2), (1, 1), (1, 3), (1, 2)))
BLOCKS = tuple(b for chunk in CHUNKS for b in chunk)
PIECES = ((0, (0, 1)), (1, (0,)), (1, (1,)))


def move(x, axis, n, step):
    return lax.ppermute(x, axis, [(i, (i + step) % n) for i in range(n)])


def swap(x, axis):
    return move(x, axis, 2, 1)


def order_body(at_ref, in_ref, out_ref):
    for h in range(4):
        first = pl.multiple_of(lax.rem(at_ref[0] + h, 4) * HD, HD)
        for s in range(3):
            out_ref[:, (3 * h + s) * HD : (3 * h + s + 1) * HD] = in_ref[s, :, pl.ds(first, HD)]


def heads_first_own(weight, x, steps=6):
    d = weight.shape[1]
    return pl.pallas_call(
        order_body,
        grid_spec=pltpu.PrefetchScalarGridSpec(
            num_scalar_prefetch=1,
            grid=(steps,),
            in_specs=[pl.BlockSpec((3, d // steps, 4 * HD), lambda k, at: (0, k, 0))],
            out_specs=pl.BlockSpec((d // steps, 12 * HD), lambda k, at: (k, 0)),
        ),
        out_shape=jax.ShapeDtypeStruct((d, 12 * HD), weight.dtype),
        name="order",
        compiler_params=pltpu.CompilerParams(vmem_limit_bytes=10 * 2**20),
    )(x, weight)


def copy_body(at_ref, in_ref, out_ref):
    out_ref[...] = in_ref[...]


def rows_first_own(weight, x):
    n = weight.shape[1]
    return pl.pallas_call(
        copy_body,
        grid_spec=pltpu.PrefetchScalarGridSpec(
            num_scalar_prefetch=1,
            grid=(4,),
            in_specs=[pl.BlockSpec((HD, n), lambda h, at: (lax.rem(at[0] + h, 4), 0))],
            out_specs=pl.BlockSpec((HD, n), lambda h, at: (h, 0)),
        ),
        out_shape=jax.ShapeDtypeStruct(weight.shape, weight.dtype),
        name="turn",
        compiler_params=pltpu.CompilerParams(vmem_limit_bytes=8 * 2**20),
    )(x, weight)


def product(lhs, rhs):
    full = jnp.dot(lhs, rhs, preferred_element_type=F32)
    return full, full.astype(BF16)


def row_of(at_ref, dz, dy, dc):
    zl, y, c = at_ref[0], at_ref[1], at_ref[2]
    return lax.rem(zl + dz, 2) * 8 + lax.rem(y + dy, 4) * 2 + lax.rem(c + dc, 2)


def attend_body(at_ref, *refs):
    n = len(PIECES)
    q_refs, k_refs, v_refs = refs[:n], refs[n : 2 * n], refs[2 * n : 3 * n]
    out_refs = refs[3 * n :]
    keys = jnp.concatenate([r[...] for r in k_refs], axis=0)
    values = jnp.concatenate([r[...] for r in v_refs], axis=0)
    lane = lax.broadcasted_iota(jnp.int32, (1, BLK), 1)
    key_pos = jnp.concatenate(
        [row_of(at_ref, dz, dy, dc) * BLK + lane for i, dcs in PIECES for dc in dcs for dz, dy in CHUNKS[i]],
        axis=1,
    )
    rank = lax.broadcasted_iota(jnp.int32, (HALF, 1), 0) + at_ref[3] * HALF
    scale = math.log2(math.e) / math.sqrt(HD)
    for q_ref, (i, dcs) in zip(q_refs, PIECES):
        rows = len(CHUNKS[i]) * HALF
        for place, dc in enumerate(dcs):
            queries = q_ref[place * rows : (place + 1) * rows]
            query_pos = jnp.concatenate([row_of(at_ref, dz, dy, dc) * BLK + rank for dz, dy in CHUNKS[i]], axis=0)
            scores = lax.dot_general(queries, keys, (((1,), (1,)), ((), ())), preferred_element_type=F32)
            scores = jnp.where(query_pos >= key_pos, scores, -1e30)
            top = jnp.max(scores, axis=1, keepdims=True)
            weights = jnp.exp2((scores - top) * scale)
            total = jnp.sum(weights, axis=1, keepdims=True)
            update = jnp.dot(weights.astype(BF16), values, preferred_element_type=F32)
            out_refs[dc][i * rows : (i + 1) * rows] = (update / total).astype(BF16)


def attention(qs, ks, vs, at):
    count = len(BLOCKS) * HALF
    return pl.pallas_call(
        attend_body,
        grid_spec=pltpu.PrefetchScalarGridSpec(
            num_scalar_prefetch=1,
            grid=(1,),
            in_specs=[pl.BlockSpec(a.shape, lambda i, at: (0, 0)) for a in (*qs, *ks, *vs)],
            out_specs=[pl.BlockSpec((count, HD), lambda i, at: (0, 0)) for _ in range(2)],
        ),
        out_shape=[jax.ShapeDtypeStruct((count, HD), BF16) for _ in range(2)],
        name="attend",
        compiler_params=pltpu.CompilerParams(vmem_limit_bytes=24 * 2**20),
    )(at, *qs, *ks, *vs)


def reduce_over_x(own, other):
    (a, a16), (z, z16) = own, other
    w = a.shape[1] // 4
    cut = lambda part, i: part[:, i * w : (i + 1) * w]
    up = move(cut(a16, 2), "x", 4, 1)
    ad = move(cut(a16, 3), "x", 4, -1)
    down = move(cut(z16, 2), "x", 4, -1)
    zu = move(cut(z16, 1), "x", 4, 1)
    mixed = (cut(a, 1) + up.astype(F32)).astype(BF16)
    au = move(mixed, "x", 4, 1)
    mixed = (cut(z, 3) + down.astype(F32)).astype(BF16)
    zd = move(mixed, "x", 4, -1)
    own_sum = cut(a, 0) + au.astype(F32) + ad.astype(F32)
    return own_sum, cut(z, 0) + zu.astype(F32) + zd.astype(F32)


def halves(q, zh):
    parts = q.reshape(-1, 2, HALF, q.shape[-1])
    low, high = parts[:, 0], parts[:, 1]
    own = jnp.where(zh == 0, low, high)
    other = jnp.where(zh == 0, high, low)
    return own.reshape(-1, q.shape[-1]), other.reshape(-1, q.shape[-1])


def reduce_over_zh(summed, zh):
    t = summed.shape[0]
    summed, zh = lax.optimization_barrier((summed, zh))
    own_q, other_q = halves(summed[:, :HD], zh)
    k, v = summed[:, HD : 2 * HD], summed[:, 2 * HD :]
    sent = jnp.concatenate([k, v, other_q]).astype(BF16)
    got = swap(sent, "zh")
    k = (k + got[:t].astype(F32)).astype(BF16)
    v = (v + got[t : 2 * t].astype(F32)).astype(BF16)
    q = (own_q + got[2 * t :].astype(F32)).astype(BF16)
    return q, k, v


def reduce_over_rows(part, rounded):
    block = {b: part[i * HALF : (i + 1) * HALF] for i, b in enumerate(BLOCKS)}
    sent = {b: rounded[i * HALF : (i + 1) * HALF] for i, b in enumerate(BLOCKS)}
    up = move(jnp.concatenate([sent[0, 1], sent[1, 1]]), "y", 4, 1)
    down = move(jnp.concatenate([sent[0, 3], sent[1, 3]]), "y", 4, -1)
    over = swap(sent[1, 2], "zl")
    first = BLOCKS.index((0, 2)) * HALF
    beyond = lax.optimization_barrier(part)[first : first + HALF]
    past = (beyond + over.astype(F32)).astype(BF16)
    far = move(past, "y", 4, 2)
    near = (block[1, 0] + up[HALF:].astype(F32) + down[HALF:].astype(F32)).astype(BF16)
    side = swap(near, "zl")
    near = block[0, 0] + up[:HALF].astype(F32) + down[:HALF].astype(F32)
    return near + far.astype(F32) + side.astype(F32)


def local(tokens, qkv_weight, out_weight):
    zl, y, c, x, zh = (lax.axis_index(a) for a in ("zl", "y", "c", "x", "zh"))
    x_at = x.reshape(1).astype(jnp.int32)
    place = jnp.stack([zl, y, c, zh]).astype(jnp.int32)
    weight = jnp.transpose(qkv_weight, (1, 0, 2))
    w_qkv = heads_first_own(weight, x_at)
    w_own = rows_first_own(out_weight, x_at)
    w_other = swap(w_own, "c")
    w_out = jnp.concatenate([w.reshape(4, HD, -1) for w in (w_own, w_other)], axis=1)
    w_out = w_out.reshape(8 * HD, -1)

    rows = {(0, 0): tokens}
    rows[1, 0] = swap(tokens, "zl")
    for dy in (1, 3, 2):
        rows[0, dy] = move(tokens, "y", 4, -dy)
    for dy in (1, 3):
        rows[1, dy] = move(rows[1, 0], "y", 4, -dy)
    rows[1, 2] = swap(rows[0, 2], "zl")

    qs, ks, vs = [], [], []
    for j, chunk in enumerate(CHUNKS):
        own = [rows[b] for b in chunk]
        other = [swap(rows[dz, dy], "c") for dz, dy in chunk]
        parts = [product(jnp.concatenate(blocks), w_qkv) for blocks in (own, other)]
        first, second = reduce_over_x(*parts)
        for summed in (jnp.concatenate([first, second]),) if j == 0 else (first, second):
            q, k, v = reduce_over_zh(summed, zh)
            qs.append(q)
            ks.append(k)
            vs.append(v)
    mine, theirs = attention(qs, ks, vs, place)

    pair = jnp.concatenate([mine, swap(theirs, "c")], axis=1)
    near = {0: pair}
    far = {0: swap(pair, "zh")}
    for dx in (1, 3, 2):
        near[dx] = move(pair, "x", 4, -dx)
    for dx in (1, 3):
        far[dx] = move(far[0], "x", 4, -dx)
    far[2] = swap(near[2], "zh")
    sums = []
    for side in (near, far):
        both = product(jnp.concatenate([side[i] for i in range(4)], axis=1), w_out)
        sums.append(lax.optimization_barrier(reduce_over_rows(*both)))
    low = jnp.where(zh == 0, sums[0], sums[1])
    high = jnp.where(zh == 0, sums[1], sums[0])
    return (tokens.astype(F32) + jnp.concatenate([low, high])).astype(BF16)


def solution(mesh):
    fine = Mesh(mesh.devices.reshape(2, 4, 2, 4, 2), ("zl", "y", "c", "x", "zh"))
    row, col = ("zl", "y", "c"), ("x", "zh")
    in_specs = (P(row, col), P(col, None, row), P(row, col))
    return jax.shard_map(local, mesh=fine, in_specs=in_specs, out_specs=P(row, col), check_vma=False)
```

```python
import math

import jax
import jax.numpy as jnp
from jax import lax
from jax.experimental import pallas as pl
from jax.experimental.pallas import tpu as pltpu
from jax.sharding import Mesh, PartitionSpec as P


HD = 128
BLK = 128
HALF = 64
F32 = jnp.float32
BF16 = jnp.bfloat16
CHUNKS = (((0, 0), (1, 0), (0, 1), (0, 3)), ((0, 2), (1, 1), (1, 3), (1, 2)))
BLOCKS = tuple(b for chunk in CHUNKS for b in chunk)
PIECES = ((0, (0, 1)), (1, (0,)), (1, (1,)))


def move(x, axis, n, step):
    return lax.ppermute(x, axis, [(i, (i + step) % n) for i in range(n)])


def swap(x, axis):
    return move(x, axis, 2, 1)


def order_body(at_ref, in_ref, out_ref):
    for h in range(4):
        first = pl.multiple_of(lax.rem(at_ref[0] + h, 4) * HD, HD)
        for s in range(3):
            out_ref[:, (3 * h + s) * HD : (3 * h + s + 1) * HD] = in_ref[s, :, pl.ds(first, HD)]


def heads_first_own(weight, x, steps=6):
    d = weight.shape[1]
    return pl.pallas_call(
        order_body,
        grid_spec=pltpu.PrefetchScalarGridSpec(
            num_scalar_prefetch=1,
            grid=(steps,),
            in_specs=[pl.BlockSpec((3, d // steps, 4 * HD), lambda k, at: (0, k, 0))],
            out_specs=pl.BlockSpec((d // steps, 12 * HD), lambda k, at: (k, 0)),
        ),
        out_shape=jax.ShapeDtypeStruct((d, 12 * HD), weight.dtype),
        name="order",
        compiler_params=pltpu.CompilerParams(vmem_limit_bytes=10 * 2**20),
    )(x, weight)


def copy_body(at_ref, in_ref, out_ref):
    out_ref[...] = in_ref[...]


def rows_first_own(weight, x):
    n = weight.shape[1]
    return pl.pallas_call(
        copy_body,
        grid_spec=pltpu.PrefetchScalarGridSpec(
            num_scalar_prefetch=1,
            grid=(4,),
            in_specs=[pl.BlockSpec((HD, n), lambda h, at: (lax.rem(at[0] + h, 4), 0))],
            out_specs=pl.BlockSpec((HD, n), lambda h, at: (h, 0)),
        ),
        out_shape=jax.ShapeDtypeStruct(weight.shape, weight.dtype),
        name="turn",
        compiler_params=pltpu.CompilerParams(vmem_limit_bytes=8 * 2**20),
    )(x, weight)


def product(lhs, rhs):
    full = jnp.dot(lhs, rhs, preferred_element_type=F32)
    return full, full.astype(BF16)


def row_of(at_ref, dz, dy, dc):
    zl, y, c = at_ref[0], at_ref[1], at_ref[2]
    return lax.rem(zl + dz, 2) * 8 + lax.rem(y + dy, 4) * 2 + lax.rem(c + dc, 2)


def attend_body(at_ref, *refs):
    n = len(PIECES)
    q_refs, k_refs, v_refs = refs[:n], refs[n : 2 * n], refs[2 * n : 3 * n]
    out_refs = refs[3 * n :]
    keys = jnp.concatenate([r[...] for r in k_refs], axis=0)
    values = jnp.concatenate([r[...] for r in v_refs], axis=0)
    lane = lax.broadcasted_iota(jnp.int32, (1, BLK), 1)
    key_pos = jnp.concatenate(
        [row_of(at_ref, dz, dy, dc) * BLK + lane for i, dcs in PIECES for dc in dcs for dz, dy in CHUNKS[i]],
        axis=1,
    )
    rank = lax.broadcasted_iota(jnp.int32, (HALF, 1), 0) + at_ref[3] * HALF
    scale = math.log2(math.e) / math.sqrt(HD)
    for q_ref, (i, dcs) in zip(q_refs, PIECES):
        rows = len(CHUNKS[i]) * HALF
        for place, dc in enumerate(dcs):
            queries = q_ref[place * rows : (place + 1) * rows]
            query_pos = jnp.concatenate([row_of(at_ref, dz, dy, dc) * BLK + rank for dz, dy in CHUNKS[i]], axis=0)
            scores = lax.dot_general(queries, keys, (((1,), (1,)), ((), ())), preferred_element_type=F32)
            scores = jnp.where(query_pos >= key_pos, scores, -1e30)
            top = jnp.max(scores, axis=1, keepdims=True)
            weights = jnp.exp2((scores - top) * scale)
            total = jnp.sum(weights, axis=1, keepdims=True)
            update = jnp.dot(weights.astype(BF16), values, preferred_element_type=F32)
            out_refs[dc][i * rows : (i + 1) * rows] = (update / total).astype(BF16)


def attention(qs, ks, vs, at):
    count = len(BLOCKS) * HALF
    return pl.pallas_call(
        attend_body,
        grid_spec=pltpu.PrefetchScalarGridSpec(
            num_scalar_prefetch=1,
            grid=(1,),
            in_specs=[pl.BlockSpec(a.shape, lambda i, at: (0, 0)) for a in (*qs, *ks, *vs)],
            out_specs=[pl.BlockSpec((count, HD), lambda i, at: (0, 0)) for _ in range(2)],
        ),
        out_shape=[jax.ShapeDtypeStruct((count, HD), BF16) for _ in range(2)],
        name="attend",
        compiler_params=pltpu.CompilerParams(vmem_limit_bytes=24 * 2**20),
    )(at, *qs, *ks, *vs)


def reduce_over_x(own, other):
    (a, a16), (z, z16) = own, other
    w = a.shape[1] // 4
    cut = lambda part, i: part[:, i * w : (i + 1) * w]
    up = move(cut(a16, 2), "x", 4, 1)
    ad = move(cut(a16, 3), "x", 4, -1)
    down = move(cut(z16, 2), "x", 4, -1)
    zu = move(cut(z16, 1), "x", 4, 1)
    mixed = (cut(a, 1) + up.astype(F32)).astype(BF16)
    au = move(mixed, "x", 4, 1)
    mixed = (cut(z, 3) + down.astype(F32)).astype(BF16)
    zd = move(mixed, "x", 4, -1)
    own_sum = cut(a, 0) + au.astype(F32) + ad.astype(F32)
    return own_sum, cut(z, 0) + zu.astype(F32) + zd.astype(F32)


def halves(q, zh):
    parts = q.reshape(-1, 2, HALF, q.shape[-1])
    low, high = parts[:, 0], parts[:, 1]
    own = jnp.where(zh == 0, low, high)
    other = jnp.where(zh == 0, high, low)
    return own.reshape(-1, q.shape[-1]), other.reshape(-1, q.shape[-1])


def reduce_over_zh(summed, zh):
    t = summed.shape[0]
    summed, zh = lax.optimization_barrier((summed, zh))
    own_q, other_q = halves(summed[:, :HD], zh)
    k, v = summed[:, HD : 2 * HD], summed[:, 2 * HD :]
    sent = jnp.concatenate([k, v, other_q]).astype(BF16)
    got = swap(sent, "zh").astype(F32)
    k = (k + got[:t]).astype(BF16)
    v = (v + got[t : 2 * t]).astype(BF16)
    q = (own_q + got[2 * t :]).astype(BF16)
    return q, k, v


def reduce_over_rows(part, rounded):
    block = {b: part[i * HALF : (i + 1) * HALF] for i, b in enumerate(BLOCKS)}
    sent = {b: rounded[i * HALF : (i + 1) * HALF] for i, b in enumerate(BLOCKS)}
    up = move(jnp.concatenate([sent[0, 1], sent[1, 1]]), "y", 4, 1)
    down = move(jnp.concatenate([sent[0, 3], sent[1, 3]]), "y", 4, -1)
    over = swap(sent[1, 2], "zl")
    first = BLOCKS.index((0, 2)) * HALF
    beyond = lax.optimization_barrier(part)[first : first + HALF]
    past = (beyond + over.astype(F32)).astype(BF16)
    far = move(past, "y", 4, 2)
    up, down = up.astype(F32), down.astype(F32)
    near = (block[1, 0] + up[HALF:] + down[HALF:]).astype(BF16)
    side = swap(near, "zl")
    return block[0, 0] + up[:HALF] + down[:HALF] + far.astype(F32) + side.astype(F32)


def local(tokens, qkv_weight, out_weight):
    zl, y, c, x, zh = (lax.axis_index(a) for a in ("zl", "y", "c", "x", "zh"))
    x_at = x.reshape(1).astype(jnp.int32)
    place = jnp.stack([zl, y, c, zh]).astype(jnp.int32)
    weight = jnp.transpose(qkv_weight, (1, 0, 2))
    w_qkv = heads_first_own(weight, x_at)
    w_own = rows_first_own(out_weight, x_at)
    w_other = swap(w_own, "c")
    w_out = jnp.concatenate([w.reshape(4, HD, -1) for w in (w_own, w_other)], axis=1)
    w_out = w_out.reshape(8 * HD, -1)

    rows = {(0, 0): tokens}
    rows[1, 0] = swap(tokens, "zl")
    for dy in (1, 3, 2):
        rows[0, dy] = move(tokens, "y", 4, -dy)
    for dy in (1, 3):
        rows[1, dy] = move(rows[1, 0], "y", 4, -dy)
    rows[1, 2] = swap(rows[0, 2], "zl")

    qs, ks, vs = [], [], []
    for j, chunk in enumerate(CHUNKS):
        own = [rows[b] for b in chunk]
        other = [swap(rows[dz, dy], "c") for dz, dy in chunk]
        parts = [product(jnp.concatenate(blocks), w_qkv) for blocks in (own, other)]
        first, second = reduce_over_x(*parts)
        for summed in (jnp.concatenate([first, second]),) if j == 0 else (first, second):
            q, k, v = reduce_over_zh(summed, zh)
            qs.append(q)
            ks.append(k)
            vs.append(v)
    mine, theirs = attention(qs, ks, vs, place)

    pair = jnp.concatenate([mine, swap(theirs, "c")], axis=1)
    near = {0: pair}
    far = {0: swap(pair, "zh")}
    for dx in (1, 3, 2):
        near[dx] = move(pair, "x", 4, -dx)
    for dx in (1, 3):
        far[dx] = move(far[0], "x", 4, -dx)
    far[2] = swap(near[2], "zh")
    sums = []
    for side in (near, far):
        both = product(jnp.concatenate([side[i] for i in range(4)], axis=1), w_out)
        sums.append(lax.optimization_barrier(reduce_over_rows(*both)))
    low = jnp.where(zh == 0, sums[0], sums[1])
    high = jnp.where(zh == 0, sums[1], sums[0])
    return (tokens.astype(F32) + jnp.concatenate([low, high])).astype(BF16)


def solution(mesh):
    fine = Mesh(mesh.devices.reshape(2, 4, 2, 4, 2), ("zl", "y", "c", "x", "zh"))
    row, col = ("zl", "y", "c"), ("x", "zh")
    in_specs = (P(row, col), P(col, None, row), P(row, col))
    return jax.shard_map(local, mesh=fine, in_specs=in_specs, out_specs=P(row, col), check_vma=False)
```

```python
import math

import jax
import jax.numpy as jnp
from jax import lax
from jax.experimental import pallas as pl
from jax.experimental.pallas import tpu as pltpu
from jax.sharding import Mesh, PartitionSpec as P


HD = 128
BLK = 128
HALF = 64
F32 = jnp.float32
BF16 = jnp.bfloat16
CHUNKS = (((0, 0), (1, 0), (0, 1), (0, 3)), ((0, 2), (1, 1), (1, 3), (1, 2)))
BLOCKS = tuple(b for chunk in CHUNKS for b in chunk)
PIECES = ((0, (0,)), (0, (1,)), (1, (0,)), (1, (1,)))


def move(x, axis, n, step):
    return lax.ppermute(x, axis, [(i, (i + step) % n) for i in range(n)])


def swap(x, axis):
    return move(x, axis, 2, 1)


def order_body(at_ref, in_ref, out_ref):
    for h in range(4):
        first = pl.multiple_of(lax.rem(at_ref[0] + h, 4) * HD, HD)
        for s in range(3):
            out_ref[:, (3 * h + s) * HD : (3 * h + s + 1) * HD] = in_ref[s, :, pl.ds(first, HD)]


def heads_first_own(weight, x, steps=6):
    d = weight.shape[1]
    return pl.pallas_call(
        order_body,
        grid_spec=pltpu.PrefetchScalarGridSpec(
            num_scalar_prefetch=1,
            grid=(steps,),
            in_specs=[pl.BlockSpec((3, d // steps, 4 * HD), lambda k, at: (0, k, 0))],
            out_specs=pl.BlockSpec((d // steps, 12 * HD), lambda k, at: (k, 0)),
        ),
        out_shape=jax.ShapeDtypeStruct((d, 12 * HD), weight.dtype),
        name="order",
        compiler_params=pltpu.CompilerParams(vmem_limit_bytes=10 * 2**20),
    )(x, weight)


def copy_body(at_ref, in_ref, out_ref):
    out_ref[...] = in_ref[...]


def rows_first_own(weight, x):
    n = weight.shape[1]
    return pl.pallas_call(
        copy_body,
        grid_spec=pltpu.PrefetchScalarGridSpec(
            num_scalar_prefetch=1,
            grid=(4,),
            in_specs=[pl.BlockSpec((HD, n), lambda h, at: (lax.rem(at[0] + h, 4), 0))],
            out_specs=pl.BlockSpec((HD, n), lambda h, at: (h, 0)),
        ),
        out_shape=jax.ShapeDtypeStruct(weight.shape, weight.dtype),
        name="turn",
        compiler_params=pltpu.CompilerParams(vmem_limit_bytes=8 * 2**20),
    )(x, weight)


def product(lhs, rhs):
    full = jnp.dot(lhs, rhs, preferred_element_type=F32)
    return full, full.astype(BF16)


def row_of(at_ref, dz, dy, dc):
    zl, y, c = at_ref[0], at_ref[1], at_ref[2]
    return lax.rem(zl + dz, 2) * 8 + lax.rem(y + dy, 4) * 2 + lax.rem(c + dc, 2)


def attend_body(at_ref, *refs):
    n = len(PIECES)
    q_refs, k_refs, v_refs = refs[:n], refs[n : 2 * n], refs[2 * n : 3 * n]
    out_refs = refs[3 * n :]
    keys = jnp.concatenate([r[...] for r in k_refs], axis=0)
    values = jnp.concatenate([r[...] for r in v_refs], axis=0)
    lane = lax.broadcasted_iota(jnp.int32, (1, BLK), 1)
    key_pos = jnp.concatenate(
        [row_of(at_ref, dz, dy, dc) * BLK + lane for i, dcs in PIECES for dc in dcs for dz, dy in CHUNKS[i]],
        axis=1,
    )
    rank = lax.broadcasted_iota(jnp.int32, (HALF, 1), 0) + at_ref[3] * HALF
    scale = math.log2(math.e) / math.sqrt(HD)
    for q_ref, (i, dcs) in zip(q_refs, PIECES):
        rows = len(CHUNKS[i]) * HALF
        for place, dc in enumerate(dcs):
            queries = q_ref[place * rows : (place + 1) * rows]
            query_pos = jnp.concatenate([row_of(at_ref, dz, dy, dc) * BLK + rank for dz, dy in CHUNKS[i]], axis=0)
            scores = lax.dot_general(queries, keys, (((1,), (1,)), ((), ())), preferred_element_type=F32)
            scores = jnp.where(query_pos >= key_pos, scores, -1e30)
            top = jnp.max(scores, axis=1, keepdims=True)
            weights = jnp.exp2((scores - top) * scale)
            total = jnp.sum(weights, axis=1, keepdims=True)
            update = jnp.dot(weights.astype(BF16), values, preferred_element_type=F32)
            out_refs[dc][i * rows : (i + 1) * rows] = (update / total).astype(BF16)


def attention(qs, ks, vs, at):
    count = len(BLOCKS) * HALF
    return pl.pallas_call(
        attend_body,
        grid_spec=pltpu.PrefetchScalarGridSpec(
            num_scalar_prefetch=1,
            grid=(1,),
            in_specs=[pl.BlockSpec(a.shape, lambda i, at: (0, 0)) for a in (*qs, *ks, *vs)],
            out_specs=[pl.BlockSpec((count, HD), lambda i, at: (0, 0)) for _ in range(2)],
        ),
        out_shape=[jax.ShapeDtypeStruct((count, HD), BF16) for _ in range(2)],
        name="attend",
        compiler_params=pltpu.CompilerParams(vmem_limit_bytes=24 * 2**20),
    )(at, *qs, *ks, *vs)


def reduce_over_x(own, other):
    (a, a16), (z, z16) = own, other
    w = a.shape[1] // 4
    cut = lambda part, i: part[:, i * w : (i + 1) * w]
    up = move(cut(a16, 2), "x", 4, 1)
    ad = move(cut(a16, 3), "x", 4, -1)
    down = move(cut(z16, 2), "x", 4, -1)
    zu = move(cut(z16, 1), "x", 4, 1)
    mixed = (cut(a, 1) + up.astype(F32)).astype(BF16)
    au = move(mixed, "x", 4, 1)
    mixed = (cut(z, 3) + down.astype(F32)).astype(BF16)
    zd = move(mixed, "x", 4, -1)
    own_sum = cut(a, 0) + au.astype(F32) + ad.astype(F32)
    return own_sum, cut(z, 0) + zu.astype(F32) + zd.astype(F32)


def halves(q, zh):
    parts = q.reshape(-1, 2, HALF, q.shape[-1])
    low, high = parts[:, 0], parts[:, 1]
    own = jnp.where(zh == 0, low, high)
    other = jnp.where(zh == 0, high, low)
    return own.reshape(-1, q.shape[-1]), other.reshape(-1, q.shape[-1])


def reduce_over_zh(summed, zh):
    t = summed.shape[0]
    summed, zh = lax.optimization_barrier((summed, zh))
    own_q, other_q = halves(summed[:, :HD], zh)
    k, v = summed[:, HD : 2 * HD], summed[:, 2 * HD :]
    sent = jnp.concatenate([k, v, other_q]).astype(BF16)
    got = swap(sent, "zh").astype(F32)
    k = (k + got[:t]).astype(BF16)
    v = (v + got[t : 2 * t]).astype(BF16)
    q = (own_q + got[2 * t :]).astype(BF16)
    return q, k, v


def reduce_over_rows(part, rounded):
    block = {b: part[i * HALF : (i + 1) * HALF] for i, b in enumerate(BLOCKS)}
    sent = {b: rounded[i * HALF : (i + 1) * HALF] for i, b in enumerate(BLOCKS)}
    up = move(jnp.concatenate([sent[0, 1], sent[1, 1]]), "y", 4, 1)
    down = move(jnp.concatenate([sent[0, 3], sent[1, 3]]), "y", 4, -1)
    over = swap(sent[1, 2], "zl")
    first = BLOCKS.index((0, 2)) * HALF
    beyond = lax.optimization_barrier(part)[first : first + HALF]
    past = (beyond + over.astype(F32)).astype(BF16)
    far = move(past, "y", 4, 2)
    up, down = up.astype(F32), down.astype(F32)
    near = (block[1, 0] + up[HALF:] + down[HALF:]).astype(BF16)
    side = swap(near, "zl")
    return block[0, 0] + up[:HALF] + down[:HALF] + far.astype(F32) + side.astype(F32)


def local(tokens, qkv_weight, out_weight):
    zl, y, c, x, zh = (lax.axis_index(a) for a in ("zl", "y", "c", "x", "zh"))
    x_at = x.reshape(1).astype(jnp.int32)
    place = jnp.stack([zl, y, c, zh]).astype(jnp.int32)
    weight = jnp.transpose(qkv_weight, (1, 0, 2))
    w_qkv = heads_first_own(weight, x_at)
    w_own = rows_first_own(out_weight, x_at)
    w_other = swap(w_own, "c")
    w_out = jnp.concatenate([w.reshape(4, HD, -1) for w in (w_own, w_other)], axis=1)
    w_out = w_out.reshape(8 * HD, -1)

    rows = {(0, 0): tokens}
    rows[1, 0] = swap(tokens, "zl")
    for dy in (1, 3, 2):
        rows[0, dy] = move(tokens, "y", 4, -dy)
    for dy in (1, 3):
        rows[1, dy] = move(rows[1, 0], "y", 4, -dy)
    rows[1, 2] = swap(rows[0, 2], "zl")

    qs, ks, vs = [], [], []
    for chunk in CHUNKS:
        own = [rows[b] for b in chunk]
        other = [swap(rows[dz, dy], "c") for dz, dy in chunk]
        parts = [product(jnp.concatenate(blocks), w_qkv) for blocks in (own, other)]
        first, second = reduce_over_x(*parts)
        for summed in (first, second):
            q, k, v = reduce_over_zh(summed, zh)
            qs.append(q)
            ks.append(k)
            vs.append(v)
    mine, theirs = attention(qs, ks, vs, place)

    pair = jnp.concatenate([mine, swap(theirs, "c")], axis=1)
    near = {0: pair}
    far = {0: swap(pair, "zh")}
    for dx in (1, 3, 2):
        near[dx] = move(pair, "x", 4, -dx)
    for dx in (1, 3):
        far[dx] = move(far[0], "x", 4, -dx)
    far[2] = swap(near[2], "zh")
    sums = []
    for side in (near, far):
        both = product(jnp.concatenate([side[i] for i in range(4)], axis=1), w_out)
        sums.append(lax.optimization_barrier(reduce_over_rows(*both)))
    low = jnp.where(zh == 0, sums[0], sums[1])
    high = jnp.where(zh == 0, sums[1], sums[0])
    return (tokens.astype(F32) + jnp.concatenate([low, high])).astype(BF16)


def solution(mesh):
    fine = Mesh(mesh.devices.reshape(2, 4, 2, 4, 2), ("zl", "y", "c", "x", "zh"))
    row, col = ("zl", "y", "c"), ("x", "zh")
    in_specs = (P(row, col), P(col, None, row), P(row, col))
    return jax.shard_map(local, mesh=fine, in_specs=in_specs, out_specs=P(row, col), check_vma=False)
```
